32 devices in a mesh: tp: 8 (over z, y), cp: 4 (over x, core).
Axes of the slice: x: 2, y: 2, z: 4, core: 2. Of those that a mesh axis runs over, the one named last changes fastest.
Arguments:
- hidden: bfloat16 [2, 512, 5120], P(None, 'cp')
- grad_out: bfloat16 [2, 512, 5120], P(None, 'cp')
- w_dq: bfloat16 [5120, 1536], replicated
- g_q: bfloat16 [1536], replicated
- w_dkv: bfloat16 [5120, 576], replicated
- g_kv: bfloat16 [512], replicated
- w_uq: bfloat16 [1536, 128, 192], P(None, 'tp')
- w_uk: bfloat16 [512, 128, 128], P(None, 'tp')
- w_uv: bfloat16 [512, 128, 128], P(None, 'tp')
- w_o: bfloat16 [128, 128, 5120], P('tp')
Outputs:
- output 1: bfloat16 [2, 512, 5120], P(None, 'cp')
- output 2: bfloat16 [2, 512, 5120], P(None, 'cp')
- output 3: float32 [5120, 1536], replicated
- output 4: float32 [1536], replicated
- output 5: float32 [5120, 576], replicated
- output 6: float32 [512], replicated
- output 7: float32 [1536, 128, 192], P(None, 'tp')
- output 8: float32 [512, 128, 128], P(None, 'tp')
- output 9: float32 [512, 128, 128], P(None, 'tp')
- output 10: float32 [128, 128, 5120], P('tp')
All inputs are finite; a program needn't handle non-finite values.
Results may differ from the reference program's by a relative error of at most 0.0163229.
Values are sent between devices in bfloat16 or wider.
A program may use at most 1 GiB of HBM per device.

```python
import jax
import jax.numpy as jnp
from jax import lax

D = 5120
HEADS = 128
Q_LORA = 1536
KV_LORA = 512
NOPE = 128
ROPE = 64
VHEAD = 128
BATCH = 2
SEQ_DEV = 128
CP = 4
QBLK = 64
THETA = 10000

SEQ = CP * SEQ_DEV
HALF_LEN = SEQ_DEV // 2
QK_DIM = NOPE + ROPE
EPS = 1e-6
NEG_BIG = -1e30


def token_positions():
    token_idx = jnp.arange(SEQ, dtype=jnp.int32)
    cp_rank = token_idx // SEQ_DEV
    local_idx = token_idx % SEQ_DEV
    block_id = jnp.where(local_idx < HALF_LEN, cp_rank, 2 * CP - 1 - cp_rank)
    return block_id * HALF_LEN + local_idx % HALF_LEN


def rope_tables(positions):
    inv_freq = 1.0 / (THETA ** (jnp.arange(ROPE // 2, dtype=jnp.float32) * 2.0 / ROPE))
    angles = positions.astype(jnp.float32)[:, None] * inv_freq[None, :]
    return jnp.cos(angles), jnp.sin(angles)


def apply_rope(values, cos_tab, sin_tab):
    half_dim = values.shape[-1] // 2
    lead_half = values[..., :half_dim]
    tail_half = values[..., half_dim:]
    return jnp.concatenate([lead_half * cos_tab - tail_half * sin_tab, tail_half * cos_tab + lead_half * sin_tab], axis=-1)


def rms_norm(raw_vals, gain_vec):
    raw_f32 = raw_vals.astype(jnp.float32)
    inv_rms = lax.rsqrt(jnp.mean(raw_f32 * raw_f32, axis=-1, keepdims=True) + EPS)
    return (raw_f32 * inv_rms * gain_vec).astype(jnp.bfloat16)


def attention(q_nope, q_pe, k_nope, k_pe, v_heads, positions):
    kn_f32 = k_nope.astype(jnp.float32)
    kp_f32 = k_pe.astype(jnp.float32)
    v_f32 = v_heads.astype(jnp.float32)
    n_blocks = SEQ // QBLK
    qn_blocks = jnp.moveaxis(q_nope.reshape(BATCH, n_blocks, QBLK, HEADS, NOPE), 1, 0)
    qp_blocks = jnp.moveaxis(q_pe.reshape(BATCH, n_blocks, QBLK, HEADS, ROPE), 1, 0)
    pos_blocks = positions.reshape(n_blocks, QBLK)

    def one_block(block_args):
        qn_blk, qp_blk, q_pos = block_args
        scores = jnp.einsum('bqhn,bkhn->bhqk', qn_blk.astype(jnp.float32), kn_f32) + jnp.einsum('bqhr,bkr->bhqk', qp_blk.astype(jnp.float32), kp_f32)
        scores = jnp.where(positions[None, :] <= q_pos[:, None], scores * QK_DIM ** -0.5, NEG_BIG)
        weights = jax.nn.softmax(scores, axis=-1)
        return jnp.einsum('bhqk,bkhv->bqhv', weights, v_f32).astype(jnp.bfloat16)

    out_blocks = lax.map(jax.checkpoint(one_block), (qn_blocks, qp_blocks, pos_blocks))
    return jnp.moveaxis(out_blocks, 0, 1).reshape(BATCH, SEQ, HEADS, VHEAD)


def forward(hidden, w_dq, g_q, w_dkv, g_kv, w_uq, w_uk, w_uv, w_o):
    positions = token_positions()
    cos_tab, sin_tab = rope_tables(positions)
    hidden_f32 = hidden.astype(jnp.float32)
    cq_raw = jnp.einsum('btd,dq->btq', hidden_f32, w_dq).astype(jnp.bfloat16)
    kv_raw = jnp.einsum('btd,dc->btc', hidden_f32, w_dkv).astype(jnp.bfloat16)
    c_q = rms_norm(cq_raw, g_q)
    c_kv = rms_norm(kv_raw[..., :KV_LORA], g_kv)
    k_pe = apply_rope(kv_raw[..., KV_LORA:].astype(jnp.float32), cos_tab, sin_tab).astype(jnp.bfloat16)
    q_all = jnp.einsum('btq,qhe->bthe', c_q.astype(jnp.float32), w_uq).astype(jnp.bfloat16)
    q_nope = q_all[..., :NOPE]
    q_pe = apply_rope(q_all[..., NOPE:].astype(jnp.float32), cos_tab[:, None, :], sin_tab[:, None, :]).astype(jnp.bfloat16)
    k_nope = jnp.einsum('btc,chn->bthn', c_kv.astype(jnp.float32), w_uk).astype(jnp.bfloat16)
    v_heads = jnp.einsum('btc,chv->bthv', c_kv.astype(jnp.float32), w_uv).astype(jnp.bfloat16)
    o_heads = attention(q_nope, q_pe, k_nope, k_pe, v_heads, positions)
    return jnp.einsum('bthv,hvd->btd', o_heads.astype(jnp.float32), w_o).astype(jnp.bfloat16)


def setup_inputs(seed: int = 0) -> dict:
    rng_keys = jax.random.split(jax.random.key(seed), 10)

    def normal_weight(rng_key, arr_shape, fan_in):
        return (jax.random.normal(rng_key, arr_shape, jnp.float32) * fan_in ** -0.5).astype(jnp.bfloat16)

    return {
        'hidden': jax.random.normal(rng_keys[0], (BATCH, SEQ, D), jnp.float32).astype(jnp.bfloat16),
        'grad_out': jax.random.normal(rng_keys[1], (BATCH, SEQ, D), jnp.float32).astype(jnp.bfloat16),
        'w_dq': normal_weight(rng_keys[2], (D, Q_LORA), D),
        'g_q': jax.random.uniform(rng_keys[3], (Q_LORA,), jnp.float32, 0.5, 1.5).astype(jnp.bfloat16),
        'w_dkv': normal_weight(rng_keys[4], (D, KV_LORA + ROPE), D),
        'g_kv': jax.random.uniform(rng_keys[5], (KV_LORA,), jnp.float32, 0.5, 1.5).astype(jnp.bfloat16),
        'w_uq': normal_weight(rng_keys[6], (Q_LORA, HEADS, QK_DIM), Q_LORA),
        'w_uk': normal_weight(rng_keys[7], (KV_LORA, HEADS, NOPE), KV_LORA),
        'w_uv': normal_weight(rng_keys[8], (KV_LORA, HEADS, VHEAD), KV_LORA),
        'w_o': normal_weight(rng_keys[9], (HEADS, VHEAD, D), HEADS * VHEAD),
    }


def reference(hidden, grad_out, w_dq, g_q, w_dkv, g_kv, w_uq, w_uk, w_uv, w_o):
    attn_out, pullback = jax.vjp(forward, hidden, w_dq.astype(jnp.float32), g_q.astype(jnp.float32), w_dkv.astype(jnp.float32), g_kv.astype(jnp.float32), w_uq.astype(jnp.float32), w_uk.astype(jnp.float32), w_uv.astype(jnp.float32), w_o.astype(jnp.float32))
    all_grads = pullback(grad_out)
    return (attn_out, all_grads[0], all_grads[1], all_grads[2], all_grads[3], all_grads[4], all_grads[5], all_grads[6], all_grads[7], all_grads[8])
```

```python
import jax
import jax.numpy as jnp
from jax import lax
from jax.sharding import PartitionSpec as P

EPS = 1e-6
THETA = 10000.0
NEG_BIG = -1e30


def layout_positions(seq_local, cp_size, cp_rank):
    half_len = seq_local // 2
    local_idx = jnp.arange(seq_local, dtype=jnp.int32)
    block_id = jnp.where(local_idx < half_len, cp_rank, 2 * cp_size - 1 - cp_rank)
    return block_id * half_len + local_idx % half_len


def rope_tables(positions, rope_dim):
    inv_freq = 1.0 / (THETA ** (jnp.arange(rope_dim // 2, dtype=jnp.float32) * 2.0 / rope_dim))
    angles = positions.astype(jnp.float32)[:, None] * inv_freq[None, :]
    return jnp.cos(angles), jnp.sin(angles)


def apply_rope(values, cos_tab, sin_tab):
    half_dim = values.shape[-1] // 2
    lead_half = values[..., :half_dim]
    tail_half = values[..., half_dim:]
    return jnp.concatenate([lead_half * cos_tab - tail_half * sin_tab, tail_half * cos_tab + lead_half * sin_tab], axis=-1)


def unrope(grad_vals, cos_tab, sin_tab):
    half_dim = grad_vals.shape[-1] // 2
    lead_half = grad_vals[..., :half_dim]
    tail_half = grad_vals[..., half_dim:]
    return jnp.concatenate([lead_half * cos_tab + tail_half * sin_tab, tail_half * cos_tab - lead_half * sin_tab], axis=-1)


def norm_f32(raw_vals, gain_vec):
    inv_rms = lax.rsqrt(jnp.mean(raw_vals * raw_vals, axis=-1, keepdims=True) + EPS)
    return raw_vals * inv_rms * gain_vec


def solution(mesh):
    cp_size = mesh.shape['cp']
    assert cp_size == 4
    f32 = jnp.float32
    bf16 = jnp.bfloat16
    chip_pairs = [(i, i ^ 2) for i in range(cp_size)]
    core_pairs = [(i, i ^ 1) for i in range(cp_size)]

    def gather_blocks(val):
        far = lax.ppermute(val, 'cp', chip_pairs)
        near = lax.ppermute(val, 'cp', core_pairs)
        far_near = lax.ppermute(far, 'cp', core_pairs)
        return [val, near, far, far_near]

    def dot(spec, lhs, rhs):
        return jnp.einsum(spec, lhs, rhs, preferred_element_type=f32)

    def per_device(hidden, grad_out, w_dq, g_q, w_dkv, g_kv, w_uq, w_uk, w_uv, w_o):
        rank = lax.axis_index('cp')
        n_batch, seq_local, d_model = hidden.shape
        q_lora = w_dq.shape[1]
        kv_lora = g_kv.shape[0]
        heads_dev, nope_dim = w_uk.shape[1:]
        qk_dim = w_uq.shape[2]
        v_dim = w_uv.shape[2]
        own_heads = heads_dev // cp_size
        seq_all = seq_local * cp_size
        score_scale = qk_dim ** -0.5
        positions = jnp.concatenate([layout_positions(seq_local, cp_size, rank ^ j) for j in range(cp_size)])
        cos_tab, sin_tab = rope_tables(positions, qk_dim - nope_dim)
        cos_own, sin_own = cos_tab[:seq_local], sin_tab[:seq_local]

        def heads_gather(val):
            blocks = gather_blocks(val)
            ordered = []
            for j, blk in enumerate(blocks):
                parts = [blk[:, (j ^ k) * seq_local:((j ^ k) + 1) * seq_local] for k in range(cp_size)]
                ordered.append(blk if j == 0 else jnp.concatenate(parts, axis=1))
            return ordered

        def heads_join(ordered, lo, hi):
            width = hi - lo
            out = jnp.zeros((n_batch, seq_all, cp_size * width), bf16)
            for j, blk in enumerate(ordered):
                out = lax.dynamic_update_slice(out, blk[..., lo:hi], (0, 0, (rank ^ j) * width))
            return out

        cq_raw = dot('btd,dq->btq', hidden, w_dq).astype(bf16)
        kv_raw = dot('btd,dc->btc', hidden, w_dkv).astype(bf16)
        cq_f32 = cq_raw.astype(f32)
        ckv_f32 = kv_raw[..., :kv_lora].astype(f32)
        gq_f32 = g_q.astype(f32)
        gkv_f32 = g_kv.astype(f32)
        c_q = norm_f32(cq_f32, gq_f32).astype(bf16)
        c_kv = norm_f32(ckv_f32, gkv_f32).astype(bf16)
        k_pe = apply_rope(kv_raw[..., kv_lora:].astype(f32), cos_own, sin_own).astype(bf16)
        latent = jnp.concatenate([c_q, c_kv, k_pe], axis=-1)
        latent_all = jnp.concatenate(gather_blocks(latent), axis=1)
        cq_all = latent_all[..., :q_lora]
        ckv_all = latent_all[..., q_lora:q_lora + kv_lora]
        kpe_all = latent_all[..., q_lora + kv_lora:]
        dy_late = lax.optimization_barrier((grad_out, latent))[0]
        dy_all = jnp.concatenate(gather_blocks(dy_late), axis=1)

        head0 = rank * own_heads
        wuq_own = lax.dynamic_slice_in_dim(w_uq, head0, own_heads, axis=1)
        wuk_own = lax.dynamic_slice_in_dim(w_uk, head0, own_heads, axis=1)
        wuv_own = lax.dynamic_slice_in_dim(w_uv, head0, own_heads, axis=1)
        wo_own = lax.dynamic_slice_in_dim(w_o, head0, own_heads, axis=0)

        q_all = dot('btq,qhe->bhte', cq_all, wuq_own).astype(bf16)
        q_pe = apply_rope(q_all[..., nope_dim:].astype(f32), cos_tab, sin_tab).astype(bf16)
        q_cat = jnp.concatenate([q_all[..., :nope_dim], q_pe], axis=-1)
        k_nope = dot('btc,chn->bhtn', ckv_all, wuk_own).astype(bf16)
        k_cat = jnp.concatenate([k_nope, jnp.broadcast_to(kpe_all[:, None], k_nope.shape[:3] + kpe_all.shape[-1:])], axis=-1)
        v_heads = dot('btc,chv->bhtv', ckv_all, wuv_own).astype(bf16)

        scores = dot('bhqe,bhke->bhqk', q_cat, k_cat)
        scores = jnp.where(positions[None, :] <= positions[:, None], scores * score_scale, NEG_BIG)
        row_max = jnp.max(scores, axis=-1, keepdims=True)
        prob = jnp.exp(scores - row_max)
        row_sum = jnp.sum(prob, axis=-1, keepdims=True)
        o_heads = (dot('bhqk,bhkv->bhqv', prob.astype(bf16), v_heads) / row_sum).astype(bf16)
        o_send = jnp.transpose(o_heads, (0, 2, 1, 3)).reshape(n_batch, seq_all, own_heads * v_dim)
        o_all = heads_join(heads_gather(o_send), 0, own_heads * v_dim)
        wo_flat = w_o.reshape(heads_dev * v_dim, d_model)
        y_part = lax.psum_scatter(dot('bte,ed->btd', o_all[:, :seq_local], wo_flat), 'tp', scatter_dimension=2, tiled=True)
        y_part = y_part.astype(bf16)

        grad_o = dot('btd,hvd->bhtv', dy_all, wo_own).astype(bf16)
        row_dot = jnp.sum(grad_o.astype(f32) * o_heads.astype(f32), axis=-1, keepdims=True)
        prob_n = prob / row_sum
        grad_v = dot('bhqk,bhqv->bkhv', prob_n.astype(bf16), grad_o).astype(bf16)
        gv_blocks = heads_gather(grad_v.reshape(n_batch, seq_all, own_heads * v_dim))
        dp = dot('bhqv,bhkv->bhqk', grad_o, v_heads)
        ds = (prob_n * (dp - row_dot) * score_scale).astype(bf16)
        dk_cat = dot('bhqk,bhqe->bkhe', ds, q_cat)
        dkn = dk_cat[..., :nope_dim].astype(bf16).reshape(n_batch, seq_all, own_heads * nope_dim)
        dkp = jnp.sum(dk_cat[..., nope_dim:], axis=2).astype(bf16)
        gk_blocks = heads_gather(jnp.concatenate([dkn, dkp], axis=-1))
        dq_cat = dot('bhqk,bhke->bqhe', ds, k_cat)
        dq_pe = unrope(dq_cat[..., nope_dim:], cos_tab[:, None, :], sin_tab[:, None, :])
        dq = jnp.concatenate([dq_cat[..., :nope_dim], dq_pe], axis=-1).astype(bf16)
        gq_blocks = heads_gather(dq.reshape(n_batch, seq_all, own_heads * qk_dim))

        gv_all = heads_join(gv_blocks, 0, own_heads * v_dim)
        gk_all = heads_join(gk_blocks, 0, own_heads * nope_dim)
        gkp_own = sum(blk[:, :seq_local, own_heads * nope_dim:].astype(f32) for blk in gk_blocks)
        dq_all = heads_join(gq_blocks, 0, own_heads * qk_dim)

        gq_own = dq_all[:, :seq_local].reshape(n_batch, seq_local, heads_dev, qk_dim)
        gk_own = gk_all[:, :seq_local].reshape(n_batch, seq_local, heads_dev, nope_dim)
        gv_own = gv_all[:, :seq_local].reshape(n_batch, seq_local, heads_dev, v_dim)
        latent_part = jnp.concatenate([
            dot('bthe,qhe->btq', gq_own, w_uq),
            dot('bthn,chn->btc', gk_own, w_uk) + dot('bthv,chv->btc', gv_own, w_uv),
            gkp_own], axis=-1)
        latent_part, y_part = lax.optimization_barrier((latent_part, y_part))
        latent_grad = lax.psum(latent_part, 'tp')
        attn_out = lax.all_gather(y_part, 'tp', axis=2, tiled=True)

        grad_cq_raw, grad_g_q = jax.vjp(norm_f32, cq_f32, gq_f32)[1](latent_grad[..., :q_lora])
        grad_ckv_raw, grad_g_kv = jax.vjp(norm_f32, ckv_f32, gkv_f32)[1](latent_grad[..., q_lora:q_lora + kv_lora])
        grad_raw = jnp.concatenate([grad_cq_raw, grad_ckv_raw, unrope(latent_grad[..., q_lora + kv_lora:], cos_own, sin_own)], axis=-1).astype(bf16)
        raw_all = jnp.concatenate(gather_blocks(grad_raw), axis=1)
        grad_hidden = (dot('btq,dq->btd', grad_raw[..., :q_lora], w_dq) + dot('btc,dc->btd', grad_raw[..., q_lora:], w_dkv)).astype(bf16)
        grad_g_q, grad_g_kv = lax.psum((grad_g_q, grad_g_kv), 'cp')

        x_late = lax.optimization_barrier((hidden, o_send))[0]
        x_all = jnp.concatenate(gather_blocks(x_late), axis=1)
        grad_w_dq = dot('btd,btq->dq', x_all, raw_all[..., :q_lora])
        grad_w_dkv = dot('btd,btc->dc', x_all, raw_all[..., q_lora:])
        grad_w_uq = dot('btq,bthe->qhe', cq_all, dq_all.reshape(n_batch, seq_all, heads_dev, qk_dim))
        grad_w_uk = dot('btc,bthn->chn', ckv_all, gk_all.reshape(n_batch, seq_all, heads_dev, nope_dim))
        grad_w_uv = dot('btc,bthv->chv', ckv_all, gv_all.reshape(n_batch, seq_all, heads_dev, v_dim))
        grad_w_o = dot('bte,btd->ed', o_all, dy_all).reshape(heads_dev, v_dim, d_model)
        return (attn_out, grad_hidden, grad_w_dq, grad_g_q, grad_w_dkv, grad_g_kv, grad_w_uq, grad_w_uk, grad_w_uv, grad_w_o)

    seq_spec = P(None, 'cp', None)
    full_spec = P()
    head_spec = P(None, 'tp', None)
    out_head_spec = P('tp', None, None)
    all_specs = (seq_spec, seq_spec, full_spec, full_spec, full_spec, full_spec, head_spec, head_spec, head_spec, out_head_spec)
    return jax.shard_map(per_device, mesh=mesh, in_specs=all_specs, out_specs=all_specs, check_vma=False)
```

```python
import jax
import jax.numpy as jnp
from jax import lax
from jax.sharding import PartitionSpec as P

EPS = 1e-6
THETA = 10000.0
NEG_BIG = -1e30


def layout_positions(seq_local, cp_size, cp_rank):
    half_len = seq_local // 2
    local_idx = jnp.arange(seq_local, dtype=jnp.int32)
    block_id = jnp.where(local_idx < half_len, cp_rank, 2 * cp_size - 1 - cp_rank)
    return block_id * half_len + local_idx % half_len


def rope_tables(positions, rope_dim):
    inv_freq = 1.0 / (THETA ** (jnp.arange(rope_dim // 2, dtype=jnp.float32) * 2.0 / rope_dim))
    angles = positions.astype(jnp.float32)[:, None] * inv_freq[None, :]
    return jnp.cos(angles), jnp.sin(angles)


def apply_rope(values, cos_tab, sin_tab):
    half_dim = values.shape[-1] // 2
    lead_half = values[..., :half_dim]
    tail_half = values[..., half_dim:]
    return jnp.concatenate([lead_half * cos_tab - tail_half * sin_tab, tail_half * cos_tab + lead_half * sin_tab], axis=-1)


def unrope(grad_vals, cos_tab, sin_tab):
    half_dim = grad_vals.shape[-1] // 2
    lead_half = grad_vals[..., :half_dim]
    tail_half = grad_vals[..., half_dim:]
    return jnp.concatenate([lead_half * cos_tab + tail_half * sin_tab, tail_half * cos_tab - lead_half * sin_tab], axis=-1)


def norm_f32(raw_vals, gain_vec):
    inv_rms = lax.rsqrt(jnp.mean(raw_vals * raw_vals, axis=-1, keepdims=True) + EPS)
    return raw_vals * inv_rms * gain_vec


def solution(mesh):
    cp_size = mesh.shape['cp']
    assert cp_size == 4
    f32 = jnp.float32
    bf16 = jnp.bfloat16
    chip_pairs = [(i, i ^ 2) for i in range(cp_size)]
    core_pairs = [(i, i ^ 1) for i in range(cp_size)]

    def gather_blocks(val):
        far = lax.ppermute(val, 'cp', chip_pairs)
        near = lax.ppermute(val, 'cp', core_pairs)
        far_near = lax.ppermute(far, 'cp', core_pairs)
        return [val, near, far, far_near]

    def dot(spec, lhs, rhs):
        return jnp.einsum(spec, lhs, rhs, preferred_element_type=f32)

    def per_device(hidden, grad_out, w_dq, g_q, w_dkv, g_kv, w_uq, w_uk, w_uv, w_o):
        rank = lax.axis_index('cp')
        n_batch, seq_local, d_model = hidden.shape
        q_lora = w_dq.shape[1]
        kv_lora = g_kv.shape[0]
        heads_dev, nope_dim = w_uk.shape[1:]
        qk_dim = w_uq.shape[2]
        v_dim = w_uv.shape[2]
        own_heads = heads_dev // cp_size
        seq_all = seq_local * cp_size
        score_scale = qk_dim ** -0.5
        positions = jnp.concatenate([layout_positions(seq_local, cp_size, rank ^ j) for j in range(cp_size)])
        cos_tab, sin_tab = rope_tables(positions, qk_dim - nope_dim)
        cos_own, sin_own = cos_tab[:seq_local], sin_tab[:seq_local]

        def heads_gather(val):
            blocks = gather_blocks(val)
            ordered = []
            for j, blk in enumerate(blocks):
                parts = [blk[:, (j ^ k) * seq_local:((j ^ k) + 1) * seq_local] for k in range(cp_size)]
                ordered.append(blk if j == 0 else jnp.concatenate(parts, axis=1))
            return ordered

        def heads_join(ordered, lo, hi):
            width = hi - lo
            out = jnp.zeros((n_batch, seq_all, cp_size * width), bf16)
            for j, blk in enumerate(ordered):
                out = lax.dynamic_update_slice(out, blk[..., lo:hi], (0, 0, (rank ^ j) * width))
            return out

        cq_raw = dot('btd,dq->btq', hidden, w_dq).astype(bf16)
        kv_raw = dot('btd,dc->btc', hidden, w_dkv).astype(bf16)
        cq_f32 = cq_raw.astype(f32)
        ckv_f32 = kv_raw[..., :kv_lora].astype(f32)
        gq_f32 = g_q.astype(f32)
        gkv_f32 = g_kv.astype(f32)
        c_q = norm_f32(cq_f32, gq_f32).astype(bf16)
        c_kv = norm_f32(ckv_f32, gkv_f32).astype(bf16)
        k_pe = apply_rope(kv_raw[..., kv_lora:].astype(f32), cos_own, sin_own).astype(bf16)
        latent = jnp.concatenate([c_q, c_kv, k_pe], axis=-1)
        latent_all = jnp.concatenate(gather_blocks(latent), axis=1)
        cq_all = latent_all[..., :q_lora]
        ckv_all = latent_all[..., q_lora:q_lora + kv_lora]
        kpe_all = latent_all[..., q_lora + kv_lora:]
        dy_late = lax.optimization_barrier((grad_out, latent))[0]
        dy_all = jnp.concatenate(gather_blocks(dy_late), axis=1)

        head0 = rank * own_heads
        wuq_own = lax.dynamic_slice_in_dim(w_uq, head0, own_heads, axis=1)
        wuk_own = lax.dynamic_slice_in_dim(w_uk, head0, own_heads, axis=1)
        wuv_own = lax.dynamic_slice_in_dim(w_uv, head0, own_heads, axis=1)
        wo_own = lax.dynamic_slice_in_dim(w_o, head0, own_heads, axis=0)

        q_all = dot('btq,qhe->bhte', cq_all, wuq_own).astype(bf16)
        q_pe = apply_rope(q_all[..., nope_dim:].astype(f32), cos_tab, sin_tab).astype(bf16)
        q_cat = jnp.concatenate([q_all[..., :nope_dim], q_pe], axis=-1)
        k_nope = dot('btc,chn->bhtn', ckv_all, wuk_own).astype(bf16)
        k_cat = jnp.concatenate([k_nope, jnp.broadcast_to(kpe_all[:, None], k_nope.shape[:3] + kpe_all.shape[-1:])], axis=-1)
        v_heads = dot('btc,chv->bhtv', ckv_all, wuv_own).astype(bf16)

        scores = dot('bhqe,bhke->bhqk', q_cat, k_cat)
        scores = jnp.where(positions[None, :] <= positions[:, None], scores * score_scale, NEG_BIG)
        row_max = jnp.max(scores, axis=-1, keepdims=True)
        prob = jnp.exp(scores - row_max)
        row_sum = jnp.sum(prob, axis=-1, keepdims=True)
        o_heads = (dot('bhqk,bhkv->bhqv', prob.astype(bf16), v_heads) / row_sum).astype(bf16)
        o_send = jnp.transpose(o_heads, (0, 2, 1, 3)).reshape(n_batch, seq_all, own_heads * v_dim)
        o_all = heads_join(heads_gather(o_send), 0, own_heads * v_dim)
        wo_flat = w_o.reshape(heads_dev * v_dim, d_model)
        y_part = lax.psum_scatter(dot('bte,ed->btd', o_all[:, :seq_local], wo_flat), 'tp', scatter_dimension=2, tiled=True)
        y_part = y_part.astype(bf16)

        grad_o = dot('btd,hvd->bhtv', dy_all, wo_own).astype(bf16)
        row_dot = jnp.sum(grad_o.astype(f32) * o_heads.astype(f32), axis=-1, keepdims=True)
        prob_n = prob / row_sum
        grad_v = dot('bhqk,bhqv->bkhv', prob_n.astype(bf16), grad_o).astype(bf16)
        gv_blocks = heads_gather(grad_v.reshape(n_batch, seq_all, own_heads * v_dim))
        dp = dot('bhqv,bhkv->bhqk', grad_o, v_heads)
        ds = (prob_n * (dp - row_dot) * score_scale).astype(bf16)
        dk_cat = dot('bhqk,bhqe->bkhe', ds, q_cat)
        dkn = dk_cat[..., :nope_dim].astype(bf16).reshape(n_batch, seq_all, own_heads * nope_dim)
        dkp = jnp.sum(dk_cat[..., nope_dim:], axis=2).astype(bf16)
        gk_blocks = heads_gather(jnp.concatenate([dkn, dkp], axis=-1))
        dq_cat = dot('bhqk,bhke->bqhe', ds, k_cat)
        dq_pe = unrope(dq_cat[..., nope_dim:], cos_tab[:, None, :], sin_tab[:, None, :])
        dq = jnp.concatenate([dq_cat[..., :nope_dim], dq_pe], axis=-1).astype(bf16)
        gq_blocks = heads_gather(dq.reshape(n_batch, seq_all, own_heads * qk_dim))

        gv_all = heads_join(gv_blocks, 0, own_heads * v_dim)
        gk_all = heads_join(gk_blocks, 0, own_heads * nope_dim)
        gkp_own = sum(blk[:, :seq_local, own_heads * nope_dim:].astype(f32) for blk in gk_blocks)
        dq_all = heads_join(gq_blocks, 0, own_heads * qk_dim)

        gq_own = dq_all[:, :seq_local].reshape(n_batch, seq_local, heads_dev, qk_dim)
        gk_own = gk_all[:, :seq_local].reshape(n_batch, seq_local, heads_dev, nope_dim)
        gv_own = gv_all[:, :seq_local].reshape(n_batch, seq_local, heads_dev, v_dim)
        latent_part = jnp.concatenate([
            dot('bthe,qhe->btq', gq_own, w_uq),
            dot('bthn,chn->btc', gk_own, w_uk) + dot('bthv,chv->btc', gv_own, w_uv),
            gkp_own], axis=-1)
        latent_part, y_part = lax.optimization_barrier((latent_part, y_part))
        latent_grad = lax.psum(latent_part, 'tp')
        attn_out = lax.all_gather(y_part, 'tp', axis=2, tiled=True)

        grad_cq_raw, grad_g_q = jax.vjp(norm_f32, cq_f32, gq_f32)[1](latent_grad[..., :q_lora])
        grad_ckv_raw, grad_g_kv = jax.vjp(norm_f32, ckv_f32, gkv_f32)[1](latent_grad[..., q_lora:q_lora + kv_lora])
        grad_raw = jnp.concatenate([grad_cq_raw, grad_ckv_raw, unrope(latent_grad[..., q_lora + kv_lora:], cos_own, sin_own)], axis=-1).astype(bf16)
        raw_all = jnp.concatenate(gather_blocks(grad_raw), axis=1)
        grad_hidden = (dot('btq,dq->btd', grad_raw[..., :q_lora], w_dq) + dot('btc,dc->btd', grad_raw[..., q_lora:], w_dkv)).astype(bf16)
        grad_g_q, grad_g_kv = lax.psum((grad_g_q, grad_g_kv), 'cp')

        x_late = lax.optimization_barrier((hidden, dq))[0]
        x_all = jnp.concatenate(gather_blocks(x_late), axis=1)
        grad_w_dq = dot('btd,btq->dq', x_all, raw_all[..., :q_lora])
        grad_w_dkv = dot('btd,btc->dc', x_all, raw_all[..., q_lora:])
        grad_w_uq = dot('btq,bthe->qhe', cq_all, dq_all.reshape(n_batch, seq_all, heads_dev, qk_dim))
        grad_w_uk = dot('btc,bthn->chn', ckv_all, gk_all.reshape(n_batch, seq_all, heads_dev, nope_dim))
        grad_w_uv = dot('btc,bthv->chv', ckv_all, gv_all.reshape(n_batch, seq_all, heads_dev, v_dim))
        grad_w_o = dot('bte,btd->ed', o_all, dy_all).reshape(heads_dev, v_dim, d_model)
        return (attn_out, grad_hidden, grad_w_dq, grad_g_q, grad_w_dkv, grad_g_kv, grad_w_uq, grad_w_uk, grad_w_uv, grad_w_o)

    seq_spec = P(None, 'cp', None)
    full_spec = P()
    head_spec = P(None, 'tp', None)
    out_head_spec = P('tp', None, None)
    all_specs = (seq_spec, seq_spec, full_spec, full_spec, full_spec, full_spec, head_spec, head_spec, head_spec, out_head_spec)
    return jax.shard_map(per_device, mesh=mesh, in_specs=all_specs, out_specs=all_specs, check_vma=False)
```
